32 devices in a mesh: job: 4 (over y, x), zero: 2 (over core), cols: 4 (over z).
Axes of the slice: x: 2, y: 2, z: 4, core: 2. Of those that a mesh axis runs over, the one named last changes fastest.
Arguments:
- weight_query: bfloat16 [12288, 3072], P(('job', 'zero'), 'cols'), parts along dimension 0, may hold values from -0.109375 to 0.109375
- low_query: bfloat16 [12288, 32], P(('job', 'zero')), parts along dimension 0, may hold values from -0.109375 to 0.109375
- high_query: bfloat16 [128, 3072], P('job', 'cols'), parts along dimension 0, may hold values from -1 to 1
- weight_key: bfloat16 [12288, 1024], P(('job', 'zero'), 'cols'), parts along dimension 0, may hold values from -0.109375 to 0.109375
- low_key: bfloat16 [12288, 32], P(('job', 'zero')), parts along dimension 0, may hold values from -0.109375 to 0.109375
- high_key: bfloat16 [128, 1024], P('job', 'cols'), parts along dimension 0, may hold values from -1 to 1
- weight_value: bfloat16 [12288, 1024], P(('job', 'zero'), 'cols'), parts along dimension 0, may hold values from -0.109375 to 0.109375
- low_value: bfloat16 [12288, 32], P(('job', 'zero')), parts along dimension 0, may hold values from -0.109375 to 0.109375
- high_value: bfloat16 [128, 1024], P('job', 'cols'), parts along dimension 0, may hold values from -1 to 1
- weight_mixed: bfloat16 [12288, 3072], P(('job', 'cols'), 'zero'), parts along dimension 0, may hold values from -0.109375 to 0.109375
- low_mixed: bfloat16 [12288, 32], P(('job', 'cols')), parts along dimension 0, may hold values from -0.109375 to 0.109375
- high_mixed: bfloat16 [128, 3072], P('job', 'zero'), parts along dimension 0, may hold values from -1 to 1
- norm_train: float32 [12288], P(('job', 'zero', 'cols')), parts along dimension 0, may hold values from 0.25 to 1.75
- norm_step: float32 [12288], P(('job', 'zero', 'cols')), parts along dimension 0, may hold values from -0.3 to 0.3
Outputs:
- serving_query: bfloat16 [12288, 3072], P('job', 'cols'), parts along dimension 0
- serving_key: bfloat16 [12288, 1024], P('job', 'cols'), parts along dimension 0
- serving_value: bfloat16 [12288, 1024], P('job', 'cols'), parts along dimension 0
- serving_mixed: bfloat16 [12288, 3072], P(('job', 'cols')), parts along dimension 0
- serve_norm: bfloat16 [12288], P('job'), parts along dimension 0
The draws below stay inside these ranges and needn't reach their ends.
There are 4 independent parts, one for each index of `job`. The reference program is written for one: setup_inputs(seed, part) draws one part's arguments, and reference() takes and returns one part's arrays. A program takes and returns all parts, laid end to end along the dimension named above; each array names one. Nothing has to cross between parts.
All inputs are finite; a program needn't handle non-finite values.
Results may differ from the reference program's by a relative error of at most 0.001.
Values may be sent and summed in bfloat16 or wider, within the bound.
A program may use at most 128 MiB of HBM per device.

```python
import jax
import jax.numpy as jnp

D_MODEL = 3072
Q_DIM = 3072
KV_DIM = 1024
RANK = 32


def shard_levels(own_key, extent, split, smallest, high):
    def one(axis_at, shards_of):
        draws = jax.random.uniform(jax.random.fold_in(jax.random.fold_in(own_key, 6), axis_at), (shards_of,), jnp.float32, smallest / len(split), high / len(split))
        return jnp.repeat(jnp.exp(draws), extent[axis_at] // shards_of).reshape((-1,) + (1,) * (len(extent) - axis_at - 1))

    loudness = one(*split[0])
    for cut in split[1:]:
        loudness = loudness * one(*cut)
    return loudness


def bell_draw(stream_key, dims, spread, most, cuts=(), dtype=jnp.bfloat16):
    gain = shard_levels(stream_key, dims, cuts, -0.22, 0.18) if cuts else 1.0
    drawn = jax.random.normal(stream_key, dims, jnp.float32) * spread * gain
    return jnp.minimum(jnp.maximum(drawn, -most), most).astype(dtype)


def setup_inputs(seed: int = 0, part: int = 0) -> dict:
    arg_keys = jax.random.split(jax.random.key(seed), 15)
    own_keys = jax.random.split(jax.random.fold_in(arg_keys[14], part), 15)
    return {
        "weight_query": bell_draw(own_keys[0], (D_MODEL, Q_DIM), D_MODEL ** -0.5, 0.109375, ((0, 2), (1, 4))),
        "low_query": bell_draw(own_keys[1], (D_MODEL, RANK), D_MODEL ** -0.5, 0.109375, ((0, 2),)),
        "high_query": bell_draw(own_keys[2], (RANK, Q_DIM), RANK ** -0.5, 1.0, ((1, 4),)),
        "weight_key": bell_draw(own_keys[3], (D_MODEL, KV_DIM), D_MODEL ** -0.5, 0.109375, ((0, 2), (1, 4))),
        "low_key": bell_draw(own_keys[4], (D_MODEL, RANK), D_MODEL ** -0.5, 0.109375, ((0, 2),)),
        "high_key": bell_draw(own_keys[5], (RANK, KV_DIM), RANK ** -0.5, 1.0, ((1, 4),)),
        "weight_value": bell_draw(own_keys[6], (D_MODEL, KV_DIM), D_MODEL ** -0.5, 0.109375, ((0, 2), (1, 4))),
        "low_value": bell_draw(own_keys[7], (D_MODEL, RANK), D_MODEL ** -0.5, 0.109375, ((0, 2),)),
        "high_value": bell_draw(own_keys[8], (RANK, KV_DIM), RANK ** -0.5, 1.0, ((1, 4),)),
        "weight_mixed": bell_draw(own_keys[9], (Q_DIM, D_MODEL), Q_DIM ** -0.5, 0.109375, ((0, 4), (1, 2))),
        "low_mixed": bell_draw(own_keys[10], (Q_DIM, RANK), Q_DIM ** -0.5, 0.109375, ((0, 4),)),
        "high_mixed": bell_draw(own_keys[11], (RANK, D_MODEL), RANK ** -0.5, 1.0, ((1, 2),)),
        "norm_train": jnp.clip(1.0 + 0.15 * jax.random.normal(own_keys[12], (D_MODEL,), jnp.float32), 0.25, 1.75),
        "norm_step": jnp.clip(jax.random.uniform(own_keys[13], (D_MODEL,), jnp.float32, -0.3, 0.3) * shard_levels(own_keys[13], (D_MODEL,), ((0, 8),), -0.4, 0.0), -0.3, 0.3),
    }


mix_rate = 2.0


def reference(weight_query, low_query, high_query, weight_key, low_key, high_key, weight_value, low_value, high_value, weight_mixed, low_mixed, high_mixed, norm_train, norm_step):
    whole_query = weight_query.astype(jnp.float32) + mix_rate * jnp.dot(low_query, high_query, preferred_element_type=jnp.float32)
    whole_key = weight_key.astype(jnp.float32) + mix_rate * jnp.dot(low_key, high_key, preferred_element_type=jnp.float32)
    whole_value = weight_value.astype(jnp.float32) + mix_rate * jnp.dot(low_value, high_value, preferred_element_type=jnp.float32)
    whole_mixed = weight_mixed.astype(jnp.float32) + mix_rate * jnp.dot(low_mixed, high_mixed, preferred_element_type=jnp.float32)
    serving_query = whole_query.astype(jnp.bfloat16)
    serving_key = whole_key.astype(jnp.bfloat16)
    serving_value = whole_value.astype(jnp.bfloat16)
    serving_mixed = whole_mixed.astype(jnp.bfloat16)
    serve_norm = (norm_train + norm_step).astype(jnp.bfloat16)
    return serving_query, serving_key, serving_value, serving_mixed, serve_norm
```

```python
import functools

import jax
import jax.numpy as jnp
from jax import lax
from jax.experimental import pallas as pl
from jax.experimental.pallas import tpu as pltpu
from jax.sharding import PartitionSpec as P


mix_rate = 2.0
lanes = 128
piece_bytes = 800 * 1024


tile_rows, tile_columns = 256, 256


def merge(done, weight, low_t, high, at, tall):
    columns = weight.shape[1]
    wide = tile_columns if columns % tile_columns == 0 else columns
    deep = tile_rows if tall % tile_rows == 0 else tall
    for top in range(at, at + tall, deep):
        low = low_t[:, pl.ds(top, deep)] * jnp.bfloat16(mix_rate)
        for left in range(0, columns, wide):
            where = (pl.ds(top, deep), pl.ds(left, wide))
            update = lax.dot_general(
                low, high[:, pl.ds(left, wide)], (((0,), (0,)), ((), ())), preferred_element_type=jnp.float32
            )
            done[where] = (weight[where].astype(jnp.float32) + update).astype(jnp.bfloat16)


def pieces_of(shape):
    rows, columns = shape
    best = lanes
    for tall in range(lanes, rows + 1, lanes):
        if rows % tall == 0 and 2 * tall * columns <= piece_bytes:
            best = tall
    return [(at, best) for at in range(0, rows, best)]


def place(whole, slot, by_rows, shape, at, tall):
    rows, columns = shape
    if by_rows:
        return whole.at[pl.ds(slot * rows + at, tall), :]
    return whole.at[pl.ds(at, tall), pl.ds(pl.multiple_of(slot * columns, lanes), columns)]


def own_kernel(by_rows, order, *refs):
    count = len(by_rows)
    weights, factors = refs[:count], refs[count : 3 * count]
    outs, lows, highs = refs[3 * count : 4 * count], refs[4 * count : 5 * count], refs[5 * count : 6 * count]
    held, done = refs[6 * count : 7 * count], refs[7 * count : 8 * count]
    read_sem, write_sem, factor_sem = refs[8 * count :]
    slot = lax.axis_index("zero")
    work = [(n, at, tall) for n in order for at, tall in pieces_of(weights[n].shape)]
    loads = []
    for i, (source, target) in enumerate(zip(factors, (*lows, *highs))):
        loads.append(pltpu.make_async_copy(source, target, factor_sem.at[i]))
        loads[-1].start()
    reads = []
    for i, (n, at, tall) in enumerate(work):
        reads.append(pltpu.make_async_copy(weights[n].at[pl.ds(at, tall), :], held[n].at[pl.ds(at, tall), :], read_sem.at[i]))
        reads[-1].start()
    for copy in loads:
        copy.wait()
    writes = []
    for i, (n, at, tall) in enumerate(work):
        reads[i].wait()
        rows = pl.ds(at, tall)
        merge(done[n], held[n], lows[n], highs[n], at, tall)
        writes.append(pltpu.make_async_copy(done[n].at[rows, :], place(outs[n], slot, by_rows[n], weights[n].shape, at, tall), write_sem.at[i]))
        writes[-1].start()
    for copy in writes:
        copy.wait()


def far_kernel(by_rows, order, parts, *refs):
    count = len(by_rows)
    weights, lows, highs = refs[:count], refs[count : 2 * count], refs[2 * count : 3 * count]
    gains = refs[4 * count : 4 * count + parts]
    refs = refs[4 * count + parts :]
    outs, gain_out, done, gain_held, write_sem = refs[:count], refs[count], refs[count + 1 : 2 * count + 1], refs[-2], refs[-1]
    slot = 1 - lax.axis_index("zero")
    work = [(n, at, tall) for n in order for at, tall in pieces_of(weights[n].shape)]
    writes = []
    for i, (n, at, tall) in enumerate(work):
        rows = pl.ds(at, tall)
        merge(done[n], weights[n], lows[n], highs[n], at, tall)
        writes.append(pltpu.make_async_copy(done[n].at[rows, :], place(outs[n], slot, by_rows[n], weights[n].shape, at, tall), write_sem.at[i]))
        writes[-1].start()
    cols, tall = lax.axis_size("cols"), gains[0].shape[0]
    for n in range(parts):
        zero = slot if n >= cols else 1 - slot
        at = zero * cols + lax.rem(lax.axis_index("cols") + cols - n % cols, cols)
        gain_held[pl.ds(at * tall, tall), :] = gains[n][...]
    gain_out[...] = gain_held[...].astype(jnp.bfloat16)
    for copy in writes:
        copy.wait()


def cost_of(weights, times):
    size = sum(w.size for w in weights)
    return pl.CostEstimate(flops=64 * size, bytes_accessed=times * size, transcendentals=0)


def paired(wq, lq, hq, wk, lk, hk, wv, lv, hv, wm, lm, hm, norm_train, norm_step):
    parts = lax.axis_size("zero") * lax.axis_size("cols")
    lq, lk, lv, lm = lq.T, lk.T, lv.T, lm.T

    def send(x, axes, perm):
        return lax.ppermute(x, axes, perm)

    swap = functools.partial(send, axes="zero", perm=[(0, 1), (1, 0)])
    gain = (norm_train + norm_step).reshape(-1, lanes)
    cols = lax.axis_size("cols")
    gains = [gain]
    for ahead in range(1, cols):
        gains.append(send(gain, "cols", [(i, (i + ahead) % cols) for i in range(cols)]))
    far_hm, far_wm = swap(hm), swap(wm)
    far_lk, far_wk = swap(lk), swap(wk)
    far_lv, far_wv = swap(lv), swap(wv)
    far_lq, far_wq = swap(lq), swap(wq)
    gains += [swap(x) for x in gains]

    by_rows = (True, True, True, False)
    order = (3, 1, 2, 0)
    weights = (wq, wk, wv, wm)
    wholes = [jax.ShapeDtypeStruct((2 * w.shape[0], w.shape[1]), w.dtype) for w in weights[:3]]
    wholes.append(jax.ShapeDtypeStruct((wm.shape[0], 2 * wm.shape[1]), wm.dtype))
    count = sum(len(pieces_of(w.shape)) for w in weights)
    memory = 2 * sum(w.size for w in weights)
    small = 8 * 2**20
    vmem, hbm = pl.BlockSpec(memory_space=pltpu.VMEM), pl.BlockSpec(memory_space=pl.ANY)
    factors = (lq, lk, lv, lm, hq, hk, hv, hm)
    far_off = lambda x: pltpu.with_memory_space_constraint(x, pltpu.HBM)
    outs = pl.pallas_call(
        functools.partial(own_kernel, by_rows, order),
        in_specs=[hbm] * 12,
        out_specs=[hbm] * 4 + [vmem] * 8,
        out_shape=wholes + [pltpu.VMEM(x.shape, x.dtype) for x in factors],
        scratch_shapes=[pltpu.VMEM(w.shape, w.dtype) for w in weights] * 2
        + [pltpu.SemaphoreType.DMA((count,))] * 2
        + [pltpu.SemaphoreType.DMA((len(factors),))],
        compiler_params=pltpu.CompilerParams(vmem_limit_bytes=2 * memory + small),
        cost_estimate=cost_of(weights, 4),
        name="own",
    )(*map(far_off, (*weights, *factors)))
    outs, (_, _, _, lm, hq, hk, hv, _) = outs[:4], outs[4:]
    near = lambda x: pltpu.with_memory_space_constraint(x, pltpu.VMEM)
    out = pl.pallas_call(
        functools.partial(far_kernel, by_rows, order, parts),
        in_specs=[vmem] * 12 + [hbm] * 4 + [vmem] * parts,
        out_specs=[hbm] * 4 + [vmem],
        out_shape=wholes + [jax.ShapeDtypeStruct((parts * gain.shape[0], lanes), jnp.bfloat16)],
        scratch_shapes=[pltpu.VMEM(w.shape, w.dtype) for w in weights]
        + [pltpu.VMEM((parts * gain.shape[0], lanes), jnp.float32), pltpu.SemaphoreType.DMA((count,))],
        input_output_aliases={12 + n: n for n in range(4)},
        compiler_params=pltpu.CompilerParams(vmem_limit_bytes=memory + small),
        cost_estimate=cost_of(weights, 2),
        name="far",
    )(
        *map(near, (far_wq, far_wk, far_wv, far_wm, far_lq, far_lk, far_lv)), near(lm),
        *map(near, (hq, hk, hv, far_hm)), *outs, *gains,
    )
    return (*out[:4], out[4].reshape(-1))


def fits(mesh, args):
    if mesh.shape["zero"] != 2:
        return False
    wq, wk, wv, wm, gain = args[0], args[3], args[6], args[9], args[12]
    split = mesh.shape["zero"] * mesh.shape["job"]
    cols = mesh.shape["cols"]
    sizes = [w.shape[0] // split for w in (wq, wk, wv)] + [w.shape[1] // cols for w in (wq, wk, wv)]
    sizes += [wm.shape[0] // (mesh.shape["job"] * cols), wm.shape[1] // 2, gain.shape[0] // (split * cols)]
    return all(size % lanes == 0 for size in sizes)


def on_device(
    weight_query,
    low_query,
    high_query,
    weight_key,
    low_key,
    high_key,
    weight_value,
    low_value,
    high_value,
    weight_mixed,
    low_mixed,
    high_mixed,
    norm_train,
    norm_step,
):
    (
        moved_query,
        moved_key,
        moved_value,
        moved_mixed,
        factor_query,
        factor_key,
        factor_value,
        factor_mixed,
    ) = (
        lax.all_gather(weight_query, "zero", axis=0, tiled=True),
        lax.all_gather(weight_key, "zero", axis=0, tiled=True),
        lax.all_gather(weight_value, "zero", axis=0, tiled=True),
        lax.all_gather(weight_mixed, "zero", axis=1, tiled=True),
        lax.all_gather(low_query, "zero", axis=0, tiled=True),
        lax.all_gather(low_key, "zero", axis=0, tiled=True),
        lax.all_gather(low_value, "zero", axis=0, tiled=True),
        lax.all_gather(high_mixed, "zero", axis=1, tiled=True),
    )
    whole_query = moved_query.astype(jnp.float32) + mix_rate * jnp.dot(
        factor_query, high_query, preferred_element_type=jnp.float32
    )
    serving_query = whole_query.astype(jnp.bfloat16)
    whole_key = moved_key.astype(jnp.float32) + mix_rate * jnp.dot(
        factor_key, high_key, preferred_element_type=jnp.float32
    )
    serving_key = whole_key.astype(jnp.bfloat16)
    whole_value = moved_value.astype(jnp.float32) + mix_rate * jnp.dot(
        factor_value, high_value, preferred_element_type=jnp.float32
    )
    serving_value = whole_value.astype(jnp.bfloat16)
    whole_mixed = moved_mixed.astype(jnp.float32) + mix_rate * jnp.dot(
        low_mixed, factor_mixed, preferred_element_type=jnp.float32
    )
    serving_mixed = whole_mixed.astype(jnp.bfloat16)
    serve_norm = lax.all_gather(
        (norm_train + norm_step).astype(jnp.bfloat16), ("zero", "cols"), axis=0, tiled=True
    )
    return (serving_query, serving_key, serving_value, serving_mixed, serve_norm)


def solution(mesh):
    placed = (
        P(("job", "zero"), "cols"),
        P(("job", "zero"), None),
        P("job", "cols"),
        P(("job", "zero"), "cols"),
        P(("job", "zero"), None),
        P("job", "cols"),
        P(("job", "zero"), "cols"),
        P(("job", "zero"), None),
        P("job", "cols"),
        P(("job", "cols"), "zero"),
        P(("job", "cols"), None),
        P("job", "zero"),
        P(("job", "zero", "cols")),
        P(("job", "zero", "cols")),
    )
    sharded = functools.partial(
        jax.shard_map,
        mesh=mesh,
        in_specs=placed,
        out_specs=(
            P("job", "cols"),
            P("job", "cols"),
            P("job", "cols"),
            P(("job", "cols"), None),
            P("job"),
        ),
        check_vma=False,
    )

    def program(*args):
        if not fits(mesh, args):
            return sharded(on_device)(*args)

        return sharded(paired)(*args)

    return program
```

```python
import functools

import jax
import jax.numpy as jnp
from jax import lax
from jax.experimental import pallas as pl
from jax.experimental.pallas import tpu as pltpu
from jax.sharding import PartitionSpec as P


mix_rate = 2.0
lanes = 128
piece_bytes = 800 * 1024


tile_rows, tile_columns = 256, 256


def merge(done, weight, low_t, high, at, tall):
    columns = weight.shape[1]
    wide = tile_columns if columns % tile_columns == 0 else columns
    deep = tile_rows if tall % tile_rows == 0 else tall
    for top in range(at, at + tall, deep):
        low = low_t[:, pl.ds(top, deep)] * jnp.bfloat16(mix_rate)
        for left in range(0, columns, wide):
            where = (pl.ds(top, deep), pl.ds(left, wide))
            update = lax.dot_general(
                low, high[:, pl.ds(left, wide)], (((0,), (0,)), ((), ())), preferred_element_type=jnp.float32
            )
            done[where] = (weight[where].astype(jnp.float32) + update).astype(jnp.bfloat16)


def pieces_of(shape):
    rows, columns = shape
    best = lanes
    for tall in range(lanes, rows + 1, lanes):
        if rows % tall == 0 and 2 * tall * columns <= piece_bytes:
            best = tall
    return [(at, best) for at in range(0, rows, best)]


def place(whole, slot, by_rows, shape, at, tall):
    rows, columns = shape
    if by_rows:
        return whole.at[pl.ds(slot * rows + at, tall), :]
    return whole.at[pl.ds(at, tall), pl.ds(pl.multiple_of(slot * columns, lanes), columns)]


def own_kernel(order, zeros, cols, *refs):
    count = len(order)
    sources = refs[:2]
    weights, factors = refs[2 : 2 + count], refs[2 + count : 2 + 3 * count]
    refs = refs[2 + 3 * count :]
    done, lows, highs, gain_out = refs[:count], refs[count : 2 * count], refs[2 * count : 3 * count], refs[3 * count]
    held, (trains, steps, train, step) = refs[3 * count + 1 : 4 * count + 1], refs[4 * count + 1 : 4 * count + 5]
    read_sem, factor_sem, send_sem, recv_sem, gain_sem = refs[4 * count + 5 :]
    first_loads = [pltpu.make_async_copy(x, y, gain_sem.at[i]) for i, (x, y) in enumerate(zip(sources, (train, step)))]
    for copy in first_loads:
        copy.start()
    work = [(n, at, tall) for n in order for at, tall in pieces_of(weights[n].shape)]
    loads = []
    for i, (source, target) in enumerate(zip(factors, (*lows, *highs))):
        loads.append(pltpu.make_async_copy(source, target, factor_sem.at[i]))
        loads[-1].start()
    reads = []
    for i, (n, at, tall) in enumerate(work):
        rows = pl.ds(at, tall)
        reads.append(pltpu.make_async_copy(weights[n].at[rows, :], held[n].at[rows, :], read_sem.at[i]))
        reads[-1].start()

    my_zero, my_col = lax.axis_index("zero"), lax.axis_index("cols")
    peers = [
        {"zero": lax.rem(my_zero + n // cols, zeros), "cols": lax.rem(my_col + n % cols, cols)}
        for n in range(zeros * cols)
    ]
    barrier = pltpu.get_barrier_semaphore()
    for peer in peers[1:]:
        pl.semaphore_signal(barrier, inc=1, device_id=peer, device_id_type=pl.DeviceIdType.MESH)
    pl.semaphore_wait(barrier, len(peers) - 1)
    for copy in first_loads:
        copy.wait()
    sends = []
    for n, peer in enumerate(peers[1:]):
        for k, (source, target) in enumerate(((train, trains), (step, steps))):
            sends.append(
                pltpu.make_async_remote_copy(
                    src_ref=source,
                    dst_ref=target.at[n],
                    send_sem=send_sem.at[2 * n + k],
                    recv_sem=recv_sem.at[2 * n + k],
                    device_id=peer,
                    device_id_type=pl.DeviceIdType.MESH,
                )
            )
            sends[-1].start()

    for copy in loads:
        copy.wait()
    for i, (n, at, tall) in enumerate(work):
        reads[i].wait()
        merge(done[n], held[n], lows[n], highs[n], at, tall)

    for copy in sends:
        copy.wait()
    tall = train.shape[0]
    for n in range(len(peers)):
        zero, col = lax.rem(my_zero + zeros - n // cols, zeros), lax.rem(my_col + cols - n % cols, cols)
        gain = train[...] + step[...] if n == 0 else trains[n - 1] + steps[n - 1]
        gain_out[pl.ds((zero * cols + col) * tall, tall), :] = gain


def far_kernel(by_rows, order, *refs):
    count = len(by_rows)
    weights, lows, highs = refs[:count], refs[count : 2 * count], refs[2 * count : 3 * count]
    own, gain, outs, gain_out = refs[3 * count : 4 * count], refs[4 * count], refs[4 * count + 1 : 5 * count + 1], refs[5 * count + 1]
    done, (own_sem, write_sem) = refs[5 * count + 2 : 6 * count + 2], refs[6 * count + 2 :]
    slot = lax.axis_index("zero")
    writes = []
    for n in order:
        rows = weights[n].shape[0]
        writes.append(pltpu.make_async_copy(own[n], place(outs[n], slot, by_rows[n], weights[n].shape, 0, rows), own_sem.at[n]))
        writes[-1].start()
    work = [(n, at, tall) for n in order for at, tall in pieces_of(weights[n].shape)]
    for i, (n, at, tall) in enumerate(work):
        merge(done[n], weights[n], lows[n], highs[n], at, tall)
        target = place(outs[n], 1 - slot, by_rows[n], weights[n].shape, at, tall)
        writes.append(pltpu.make_async_copy(done[n].at[pl.ds(at, tall), :], target, write_sem.at[i]))
        writes[-1].start()
    gain_out[...] = gain[...].astype(jnp.bfloat16)
    for copy in writes:
        copy.wait()


def cost_of(weights, times):
    size = sum(w.size for w in weights)
    return pl.CostEstimate(flops=64 * size, bytes_accessed=times * size, transcendentals=0)


def paired(wq, lq, hq, wk, lk, hk, wv, lv, hv, wm, lm, hm, norm_train, norm_step):
    zeros, cols = lax.axis_size("zero"), lax.axis_size("cols")
    peers = zeros * cols - 1
    lq, lk, lv, lm = lq.T, lk.T, lv.T, lm.T

    def swap(x):
        return lax.ppermute(x, "zero", [(0, 1), (1, 0)])

    far_hm, far_wm = swap(hm), swap(wm)
    far_lk, far_wk = swap(lk), swap(wk)
    far_lv, far_wv = swap(lv), swap(wv)
    far_lq, far_wq = swap(lq), swap(wq)

    by_rows = (True, True, True, False)
    order = (3, 1, 2, 0)
    weights = (wq, wk, wv, wm)
    wholes = [jax.ShapeDtypeStruct((2 * w.shape[0], w.shape[1]), w.dtype) for w in weights[:3]]
    wholes.append(jax.ShapeDtypeStruct((wm.shape[0], 2 * wm.shape[1]), wm.dtype))
    count = sum(len(pieces_of(w.shape)) for w in weights)
    memory = 2 * sum(w.size for w in weights)
    small = 8 * 2**20
    vmem, hbm = pl.BlockSpec(memory_space=pltpu.VMEM), pl.BlockSpec(memory_space=pl.ANY)
    factors = (lq, lk, lv, lm, hq, hk, hv, hm)
    far_off = lambda x: pltpu.with_memory_space_constraint(x, pltpu.HBM)
    train, step = norm_train.reshape(-1, lanes), norm_step.reshape(-1, lanes)
    whole_gain = ((peers + 1) * train.shape[0], lanes)
    *own, own_lq, own_lk, own_lv, own_lm, own_hq, own_hk, own_hv, own_hm, gain = pl.pallas_call(
        functools.partial(own_kernel, order, zeros, cols),
        in_specs=[hbm] * 14,
        out_specs=[vmem] * 13,
        out_shape=[pltpu.VMEM(x.shape, x.dtype) for x in (*weights, *factors)] + [pltpu.VMEM(whole_gain, jnp.float32)],
        scratch_shapes=[pltpu.VMEM(w.shape, w.dtype) for w in weights]
        + [pltpu.VMEM((peers, *train.shape), train.dtype)] * 2
        + [pltpu.VMEM(train.shape, train.dtype)] * 2
        + [pltpu.SemaphoreType.DMA((count,)), pltpu.SemaphoreType.DMA((len(factors),))]
        + [pltpu.SemaphoreType.DMA((2 * peers,))] * 2
        + [pltpu.SemaphoreType.DMA((2,))],
        compiler_params=pltpu.CompilerParams(
            vmem_limit_bytes=memory + small, collective_id=0, has_side_effects=True
        ),
        cost_estimate=cost_of(weights, 2),
        name="own",
    )(*map(far_off, (train, step, *weights, *factors)))
    near = lambda x: pltpu.with_memory_space_constraint(x, pltpu.VMEM)
    out = pl.pallas_call(
        functools.partial(far_kernel, by_rows, order),
        in_specs=[vmem] * 17,
        out_specs=[hbm] * 4 + [vmem],
        out_shape=wholes + [jax.ShapeDtypeStruct(whole_gain, jnp.bfloat16)],
        scratch_shapes=[pltpu.VMEM(w.shape, w.dtype) for w in weights]
        + [pltpu.SemaphoreType.DMA((len(weights),)), pltpu.SemaphoreType.DMA((count,))],
        compiler_params=pltpu.CompilerParams(vmem_limit_bytes=memory + small),
        cost_estimate=cost_of(weights, 4),
        name="far",
    )(
        *map(near, (far_wq, far_wk, far_wv, far_wm, far_lq, far_lk, far_lv, own_lm)),
        *map(near, (own_hq, own_hk, own_hv, far_hm, *own, gain)),
    )
    return (*out[:4], out[4].reshape(-1))


def fits(mesh, args):
    if mesh.shape["zero"] != 2:
        return False
    wq, wk, wv, wm, gain = args[0], args[3], args[6], args[9], args[12]
    split = mesh.shape["zero"] * mesh.shape["job"]
    cols = mesh.shape["cols"]
    sizes = [w.shape[0] // split for w in (wq, wk, wv)] + [w.shape[1] // cols for w in (wq, wk, wv)]
    sizes += [wm.shape[0] // (mesh.shape["job"] * cols), wm.shape[1] // 2, gain.shape[0] // (split * cols)]
    return all(size % lanes == 0 for size in sizes)


def on_device(
    weight_query,
    low_query,
    high_query,
    weight_key,
    low_key,
    high_key,
    weight_value,
    low_value,
    high_value,
    weight_mixed,
    low_mixed,
    high_mixed,
    norm_train,
    norm_step,
):
    (
        moved_query,
        moved_key,
        moved_value,
        moved_mixed,
        factor_query,
        factor_key,
        factor_value,
        factor_mixed,
    ) = (
        lax.all_gather(weight_query, "zero", axis=0, tiled=True),
        lax.all_gather(weight_key, "zero", axis=0, tiled=True),
        lax.all_gather(weight_value, "zero", axis=0, tiled=True),
        lax.all_gather(weight_mixed, "zero", axis=1, tiled=True),
        lax.all_gather(low_query, "zero", axis=0, tiled=True),
        lax.all_gather(low_key, "zero", axis=0, tiled=True),
        lax.all_gather(low_value, "zero", axis=0, tiled=True),
        lax.all_gather(high_mixed, "zero", axis=1, tiled=True),
    )
    whole_query = moved_query.astype(jnp.float32) + mix_rate * jnp.dot(
        factor_query, high_query, preferred_element_type=jnp.float32
    )
    serving_query = whole_query.astype(jnp.bfloat16)
    whole_key = moved_key.astype(jnp.float32) + mix_rate * jnp.dot(
        factor_key, high_key, preferred_element_type=jnp.float32
    )
    serving_key = whole_key.astype(jnp.bfloat16)
    whole_value = moved_value.astype(jnp.float32) + mix_rate * jnp.dot(
        factor_value, high_value, preferred_element_type=jnp.float32
    )
    serving_value = whole_value.astype(jnp.bfloat16)
    whole_mixed = moved_mixed.astype(jnp.float32) + mix_rate * jnp.dot(
        low_mixed, factor_mixed, preferred_element_type=jnp.float32
    )
    serving_mixed = whole_mixed.astype(jnp.bfloat16)
    serve_norm = lax.all_gather(
        (norm_train + norm_step).astype(jnp.bfloat16), ("zero", "cols"), axis=0, tiled=True
    )
    return (serving_query, serving_key, serving_value, serving_mixed, serve_norm)


def solution(mesh):
    placed = (
        P(("job", "zero"), "cols"),
        P(("job", "zero"), None),
        P("job", "cols"),
        P(("job", "zero"), "cols"),
        P(("job", "zero"), None),
        P("job", "cols"),
        P(("job", "zero"), "cols"),
        P(("job", "zero"), None),
        P("job", "cols"),
        P(("job", "cols"), "zero"),
        P(("job", "cols"), None),
        P("job", "zero"),
        P(("job", "zero", "cols")),
        P(("job", "zero", "cols")),
    )
    sharded = functools.partial(
        jax.shard_map,
        mesh=mesh,
        in_specs=placed,
        out_specs=(
            P("job", "cols"),
            P("job", "cols"),
            P("job", "cols"),
            P(("job", "cols"), None),
            P("job"),
        ),
        check_vma=False,
    )

    def program(*args):
        if not fits(mesh, args):
            return sharded(on_device)(*args)

        return sharded(paired)(*args)

    return program
```
